32 devices in a mesh: seq: 8 (over z, x), batch: 4 (over y, core).
Axes of the slice: x: 2, y: 2, z: 4, core: 2. Of those that a mesh axis runs over, the one named last changes fastest.
Arguments:
- hidden: bfloat16 [8, 2048, 4096], P('batch', None, 'seq')
- gain: float32 [4096], P('seq'), may hold values from 0.5 to 1.5
- value_weight: float32 [4096], P('seq'), may hold values from -0.09375 to 0.09375
- rewards: float32 [8, 2048], P('batch', 'seq'), may hold values from -1.5 to 1.5
- reward_mask: int32 [8, 2048], P('batch', 'seq'), may hold values 0 or 1
- lengths: int32 [8], P('batch'), may hold values from 512 to 2048
- horizon: float32 [8], P('batch'), may hold values from 24 to 16384
Outputs:
- advantages: float32 [8, 2048], P(None, ('seq', 'batch'))
- returns: float32 [8, 2048], P(None, ('seq', 'batch'))
The draws below stay inside these ranges and needn't reach their ends.
All inputs are finite; a program needn't handle non-finite values. No bound on the sum of `reward_mask` on one device may be relied on, other than what follows from the above.
Results may differ from the reference program's by a relative error of at most 0.0003.
Values may be sent and summed in bfloat16 or wider, within the bound.
A program may use at most 64 MiB of HBM per device.

```python
import jax
import jax.numpy as jnp
from jax import lax

D = 4096
B = 8
S = 2048


def draw_hidden(key, part):
    first_key = jax.random.fold_in(key, 11)
    second_key = jax.random.fold_in(key, 12)
    base = jax.random.normal(first_key, (B, S, D), jnp.float32)
    scales = jnp.exp(jax.random.uniform(second_key, (B, S, D // 16, 1), jnp.float32, -1.2, 1.2))
    return (base.reshape(B, S, D // 16, 16) * scales).reshape(B, S, D).astype(jnp.bfloat16)


def draw_horizon(key, part):
    inner = jax.random.fold_in(key, 21)
    lower = jnp.log(24.0)
    upper = jnp.log(4.0 * S)
    return jnp.exp(jax.random.uniform(inner, (B,), jnp.float32, lower, upper)).astype(jnp.float32)


def place_ends(drawn, rng, least, high):
    dims = drawn.shape
    index_at = [jax.random.randint(jax.random.fold_in(rng, axis), (), 0, dims[axis]) for axis in range(len(dims))]
    drawn = drawn.at[tuple(index_at)].set(least)
    longest = dims.index(max(dims))
    index_at[longest] = (index_at[longest] + 1) % dims[longest]
    return drawn.at[tuple(index_at)].set(high)


def level_of(key, dims, shards, low, high):
    factor_of = 1.0
    for axis_at, parts in shards:
        steps = jax.random.uniform(jax.random.fold_in(jax.random.fold_in(key, 6), axis_at), (parts,), jnp.float32, low / len(shards), high / len(shards))
        factor_of = factor_of * jnp.repeat(jnp.exp(steps), dims[axis_at] // parts).reshape((-1,) + (1,) * (len(dims) - 1 - axis_at))
    return factor_of


def normal_values(own_key, dims, scale, limit, split=(), held_as=jnp.bfloat16):
    result = scale * jax.random.normal(own_key, dims, jnp.float32)
    if split:
        result = result * level_of(own_key, dims, split, -0.22, 0.18)
    return jnp.clip(result, -limit, limit).astype(held_as)


def setup_inputs(seed: int = 0) -> dict:
    splits = jax.random.split(jax.random.key(seed), 8)
    return {
        "hidden": draw_hidden(jax.random.fold_in(splits[7], 71), 0),
        "gain": jnp.clip(1.0 + 0.1 * jax.random.normal(splits[1], (D,), jnp.float32), 0.5, 1.5),
        "value_weight": normal_values(splits[2], (D,), D ** -0.5, 0.09375, ((0, 8),), jnp.float32),
        "rewards": normal_values(splits[3], (B, S), 0.1, 1.5, ((0, 4), (1, 8)), jnp.float32),
        "reward_mask": place_ends((jax.random.randint(splits[4], (B, S), 0, 4) < 1).astype(jnp.int32), jax.random.fold_in(splits[4], 1), 0, 1),
        "lengths": place_ends(jax.random.randint(splits[5], (B,), S // 4, S + 1), jax.random.fold_in(splits[5], 1), S // 4, S).astype(jnp.int32),
        "horizon": draw_horizon(jax.random.fold_in(splits[7], 71), 0),
    }


EPS = 1e-05

def reference(hidden, gain, value_weight, rewards, reward_mask, lengths, horizon):
    head_vec = gain * value_weight

    def head(rows):
        wide_rows = rows.astype(jnp.float32)
        return lax.optimization_barrier(jnp.sum(wide_rows * head_vec, -1)) * lax.rsqrt(lax.optimization_barrier(jnp.mean(wide_rows * wide_rows, -1)) + EPS)
    values = lax.map(head, hidden)
    length_all = hidden.shape[1]
    positions = jnp.arange(length_all, dtype=jnp.int32)
    valid = (positions[None, :] < lengths[:, None]).astype(jnp.float32)
    next_valid = (positions[None, :] + 1 < lengths[:, None]).astype(jnp.float32)
    next_values = jnp.concatenate([values[:, 1:], jnp.zeros((values.shape[0], 1), jnp.float32)], 1)
    delta = (rewards * reward_mask.astype(jnp.float32) + next_valid * next_values - values) * valid
    decay = jnp.exp(-1.0 / horizon)

    def step(carry, inputs):
        d_now, v_next = inputs
        fresh = d_now + decay * v_next * carry
        return (fresh, fresh)
    _, gae_t = lax.scan(step, jnp.zeros(values.shape[0], jnp.float32), (delta.T, next_valid.T), reverse=True)
    gae = gae_t.T
    returns = (gae + values) * valid
    count = jnp.sum(valid)
    first = jnp.sum(gae)
    second = jnp.sum(gae * gae)
    mean = first / count
    var = jnp.maximum(second / count - mean * mean, 1.0)
    advantages = (gae - mean) * valid * lax.rsqrt(var)
    return (advantages, returns)
```

```python
import functools

import jax
import jax.numpy as jnp
from jax import lax
from jax.experimental import pallas as pl
from jax.experimental.pallas import tpu as pltpu
from jax.sharding import PartitionSpec as P

EPS = 1e-05
LANES = 128
F32 = jnp.float32


def kernel(n, nb, owners, hidden, gain, weight, rewards, mask, lengths, horizon,
           adv_ref, ret_ref,
           hv, gain_v, weight_v, rew_v, mask_v, len_s, hor_s,
           part, rbuf, rw_send, rw_recv, len_send, len_recv, hor_send, hor_recv,
           sum_send, sum_recv, tok_send, tok_recv,
           chunk_sem, small_sem, part_ss, part_rs, rw_ss, rw_rs, info_ss, info_rs,
           sum_ss, sum_rs, tok_ss, tok_rs):
    R, T, depth = hidden.shape
    block = rewards.shape[1]
    width = block // nb
    per = n // owners
    base = (n - owners) // 2
    L = T // owners
    G = L // LANES
    gb = block // LANES
    rows = G * R
    total = depth * n
    everyone = n * nb
    s = lax.axis_index("seq")
    b = lax.axis_index("batch")
    is_owner = (s >= base) & (s < base + owners)
    mine = s - base
    out_o = s // per
    rw_at = base + out_o
    half = s % per

    def chunk_copy(o):
        span = pl.ds(o * L, L)
        return pltpu.make_async_copy(hidden.at[:, span, :], hv.at[:, span, :], chunk_sem.at[o])

    smalls = [
        pltpu.make_async_copy(src, dst, small_sem.at[i])
        for i, (src, dst) in enumerate(
            ((gain, gain_v), (weight, weight_v), (rewards, rew_v), (mask, mask_v),
             (lengths, len_s), (horizon, hor_s)))
    ]
    for copy in smalls:
        copy.start()
    for o in range(owners):
        chunk_copy(o).start()
    barrier = pltpu.get_barrier_semaphore()
    for k in range(1, n):
        pl.semaphore_signal(barrier, inc=1, device_id={"seq": (s + k) % n},
                            device_id_type=pl.DeviceIdType.MESH)
    for k in range(1, nb):
        pl.semaphore_signal(barrier, inc=1, device_id={"batch": (b + k) % nb},
                            device_id_type=pl.DeviceIdType.MESH)
    for copy in smalls:
        copy.wait()

    head = (gain_v[...] * weight_v[...]).reshape(1, depth)
    high = head.astype(jnp.bfloat16).astype(F32)
    middle = (head - high).astype(jnp.bfloat16).astype(F32)
    low = head - high - middle
    wrow = lax.broadcasted_iota(jnp.int32, (16, depth), 0)
    pieces = jnp.where(wrow == 0, high, jnp.where(wrow == 1, middle, jnp.where(wrow == 2, low, 0.0)))
    pieces = pieces.astype(jnp.bfloat16)

    rw = rew_v[...] * mask_v[...].astype(F32)
    for g in range(gb):
        rw_send[g * R:(g + 1) * R, :] = rw[:, g * LANES:(g + 1) * LANES]
    for r in range(R):
        len_send[r:r + 1, :] = jnp.full((1, LANES), len_s[r], jnp.int32)
        hor_send[r:r + 1, :] = jnp.full((1, LANES), hor_s[r], F32)

    diagonal = (lax.broadcasted_iota(jnp.int32, (LANES, LANES), 0)
                == lax.broadcasted_iota(jnp.int32, (LANES, LANES), 1))

    def compute(o, carry):
        chunk_copy(o).wait()
        for g in range(G):
            for r in range(R):
                at = pl.ds(pl.multiple_of(o * L + g * LANES, LANES), LANES)
                h = hv[r, at, :]
                both = lax.dot_general(jnp.concatenate([h, pieces], 0), h,
                                       (((1,), (1,)), ((), ())), preferred_element_type=F32)
                row = g * R + r
                part[o, 0, row:row + 1, :] = jnp.sum(both[LANES:LANES + 8], 0, keepdims=True)
                part[o, 1, row:row + 1, :] = jnp.sum(
                    jnp.where(diagonal, both[:LANES], 0.0), 0, keepdims=True)
        return carry

    lax.fori_loop(0, owners, compute, 0)

    pl.semaphore_wait(barrier, n - 1 + nb - 1)

    def part_copy(o):
        return pltpu.make_async_remote_copy(
            part.at[o], rbuf.at[s], part_ss.at[o], part_rs.at[s],
            device_id={"seq": base + o}, device_id_type=pl.DeviceIdType.MESH)

    def rw_copy():
        return pltpu.make_async_remote_copy(
            rw_send, rw_recv.at[half], rw_ss, rw_rs.at[half],
            device_id={"seq": rw_at}, device_id_type=pl.DeviceIdType.MESH)

    for o in range(owners):
        @pl.when(base + o != s)
        def _():
            part_copy(o).start()

    @pl.when(rw_at != s)
    def _():
        rw_copy().start()

    @pl.when(rw_at == s)
    def _():
        rw_recv[half] = rw_send[...]

    infos = []
    for k in range(1, nb):
        for i, (src, dst) in enumerate(((len_send, len_recv), (hor_send, hor_recv))):
            infos.append((k, i, src, dst))

    def info_copy(k, i, src, dst):
        return pltpu.make_async_remote_copy(
            src, dst.at[b], info_ss.at[i, k], info_rs.at[i, b],
            device_id={"batch": (b + k) % nb}, device_id_type=pl.DeviceIdType.MESH)

    def info_arrived(k, i, src, dst):
        at = (b + k) % nb
        return pltpu.make_async_remote_copy(
            src, dst.at[at], info_ss.at[i, k], info_rs.at[i, at],
            device_id={"batch": at}, device_id_type=pl.DeviceIdType.MESH)

    for entry in infos:
        info_copy(*entry).start()
    len_recv[b] = len_send[...]
    hor_recv[b] = hor_send[...]

    def sum_copy(k):
        to = (s * nb + b + k) % everyone
        return pltpu.make_async_remote_copy(
            sum_send, sum_recv.at[mine, b], sum_ss.at[k], sum_rs.at[mine, b],
            device_id={"seq": to // nb, "batch": to % nb}, device_id_type=pl.DeviceIdType.MESH)

    def tok_copy(h, c):
        g = h * gb + (c * width) // LANES
        return pltpu.make_async_remote_copy(
            tok_send.at[g], tok_recv.at[b], tok_ss.at[h, c], tok_rs.at[b],
            device_id={"seq": mine * per + h, "batch": c}, device_id_type=pl.DeviceIdType.MESH)

    @pl.when(is_owner)
    def _():
        row = lax.broadcasted_iota(jnp.int32, (rows, LANES), 0)
        lane = lax.broadcasted_iota(jnp.int32, (rows, LANES), 1)
        group = row // R
        which = row % R
        length = jnp.full((rows, LANES), len_s[0], jnp.int32)
        reach = jnp.full((rows, LANES), hor_s[0], F32)
        for r in range(1, R):
            length = jnp.where(which == r, len_s[r], length)
            reach = jnp.where(which == r, hor_s[r], reach)
        rate = -1.0 / reach
        local = group * LANES + lane
        token = mine * L + local
        valid = (token < length).astype(F32)
        next_valid = (token + 1 < length).astype(F32)
        steps = [1 << i for i in range(LANES.bit_length() - 1)]
        lane_decay = [jnp.where(lane < LANES - k, jnp.exp(rate * k), 0.0) for k in steps]
        hops = [1 << i for i in range(max(G - 1, 0).bit_length())]
        row_decay = [jnp.where(group + k < G, jnp.exp(rate * (k * LANES)), 0.0) for k in hops]
        into = jnp.where(group < G - 1, jnp.exp(rate * (LANES - lane).astype(F32)), 0.0)
        power = jnp.exp(rate * (L - 1 - local).astype(F32))
        decay = jnp.exp(rate)
        power_sum = jnp.sum(power, 1, keepdims=True)
        power_squares = jnp.sum(power * power, 1, keepdims=True)

        for h in range(per):
            @pl.when(mine * per + h != s)
            def _():
                pltpu.make_async_remote_copy(
                    rw_send, rw_recv.at[h], rw_ss, rw_rs.at[h],
                    device_id={"seq": s}, device_id_type=pl.DeviceIdType.MESH).wait_recv()
        gains = jnp.concatenate([rw_recv[h] for h in range(per)], 0)

        rbuf[s] = part[mine]
        for k in range(1, n):
            at = (s + k) % n
            pltpu.make_async_remote_copy(
                part.at[0], rbuf.at[at], part_ss.at[0], part_rs.at[at],
                device_id={"seq": at}, device_id_type=pl.DeviceIdType.MESH).wait_recv()
        projected = rbuf[0, 0]
        squares = rbuf[0, 1]
        for k in range(1, n):
            projected = projected + rbuf[k, 0]
            squares = squares + rbuf[k, 1]
        values = projected * lax.rsqrt(squares / total + EPS)
        ahead = pltpu.roll(values, LANES - 1, 1)
        if G > 1:
            after = jnp.where(group < G - 1, pltpu.roll(ahead, rows - R, 0), 0.0)
        else:
            after = jnp.zeros_like(ahead)
        next_values = jnp.where(lane == LANES - 1, after, ahead)
        gae = (gains + next_valid * next_values - values) * valid
        for k, factor in zip(steps, lane_decay):
            gae = gae + factor * pltpu.roll(gae, LANES - k, 1)
        if G > 1:
            start = jnp.broadcast_to(gae[:, 0:1], (rows, LANES))
            for k, factor in zip(hops, row_decay):
                start = start + factor * pltpu.roll(start, rows - k * R, 0)
            gae = gae + into * pltpu.roll(start, rows - R, 0)
        for g in range(G):
            tok_send[g, 0] = gae[g * R:(g + 1) * R]
            tok_send[g, 1] = values[g * R:(g + 1) * R]
        for h in range(per):
            for c in range(nb):
                self_copy = (mine * per + h == s) & (b == c)

                @pl.when(jnp.logical_not(self_copy))
                def _():
                    tok_copy(h, c).start()

                @pl.when(self_copy)
                def _():
                    tok_recv[b] = tok_send[h * gb + (c * width) // LANES]
        sums = jnp.where(lane == 1, jnp.sum(gae, 1, keepdims=True), 0.0)
        sums = jnp.where(lane == 2, 2.0 * jnp.sum(gae * power, 1, keepdims=True), sums)
        sums = jnp.where(lane == 3, jnp.sum(gae * gae, 1, keepdims=True), sums)
        sums = jnp.where(lane == 4, power_sum, sums)
        sums = jnp.where(lane == 5, power_squares, sums)
        sums = jnp.where((lane == 0) & (group == 0), values + decay * gae, sums)
        summary = sums[0:R]
        for g in range(1, G):
            summary = summary + sums[g * R:(g + 1) * R]
        sum_send[...] = summary
        sum_recv[mine, b] = summary
        if everyone <= 32:
            for k in range(1, everyone):
                sum_copy(k).start()
        else:
            def start(k, carry):
                sum_copy(k).start()
                return carry
            lax.fori_loop(1, everyone, start, 0)

    for entry in infos:
        info_arrived(*entry).wait_recv()
    lane = lax.broadcasted_iota(jnp.int32, (R, LANES), 1)
    group_out = half * gb + (b * width) // LANES
    local = group_out * LANES + lane
    token = out_o * L + local
    count = jnp.zeros((R, LANES), F32)
    jump, power_out, valid_out, lens = [], [], [], []
    for c in range(nb):
        length = len_recv[c]
        rate = -1.0 / hor_recv[c]
        count = count + jnp.minimum(length, T).astype(F32)
        jump.append(jnp.exp(rate * float(L)))
        power_out.append(jnp.exp(rate * (L - 1 - local).astype(F32)))
        valid_out.append((token < length).astype(F32))
        lens.append(length)
    count = jnp.sum(count, 0, keepdims=True)

    for o in range(owners):
        for c in range(nb):
            @pl.when((base + o != s) | (b != c))
            def _():
                pltpu.make_async_remote_copy(
                    sum_send, sum_recv.at[o, c], sum_ss.at[0], sum_rs.at[o, c],
                    device_id={"seq": base + o, "batch": c},
                    device_id_type=pl.DeviceIdType.MESH).wait_recv()

    acc = jnp.zeros((R, LANES), F32)
    entering = []
    for c in range(nb):
        u = jnp.zeros((R, LANES), F32)
        chosen = jnp.zeros((R, LANES), F32)
        for o in reversed(range(owners)):
            message = sum_recv[o, c]
            factor = jnp.where((lane == 1) | (lane == 3), 1.0,
                               jnp.where((lane == 2) | (lane == 4), u,
                                         jnp.where(lane == 5, u * u, 0.0)))
            acc = acc + message * factor
            chosen = jnp.where(out_o == o, u, chosen)
            if o:
                first_value = jnp.broadcast_to(message[:, 0:1], (R, LANES))
                u = jnp.where(o * L < lens[c], first_value + jump[c] * u, 0.0)
        entering.append(chosen)
    acc = jnp.sum(acc, 0, keepdims=True)
    lane1 = lax.broadcasted_iota(jnp.int32, (1, LANES), 1)
    first = jnp.sum(jnp.where((lane1 == 1) | (lane1 == 4), acc, 0.0), 1, keepdims=True)
    second = jnp.sum(jnp.where((lane1 == 2) | (lane1 == 3) | (lane1 == 5), acc, 0.0), 1, keepdims=True)
    mean = first / count
    var = jnp.maximum(second / count - mean * mean, 1.0)
    scale = lax.rsqrt(var)

    for c in range(nb):
        @pl.when((rw_at != s) | (b != c))
        def _():
            pltpu.make_async_remote_copy(
                tok_send.at[0], tok_recv.at[c], tok_ss.at[0, 0], tok_rs.at[c],
                device_id={"seq": rw_at, "batch": c},
                device_id_type=pl.DeviceIdType.MESH).wait_recv()
    spots = LANES // width
    spot = b % spots

    def pick(x):
        result = x[:, 0:width]
        for j in range(1, spots):
            result = jnp.where(spot == j, x[:, j * width:(j + 1) * width], result)
        return result

    for c in range(nb):
        gae = tok_recv[c, 0] + power_out[c] * entering[c]
        ret_ref[c * R:(c + 1) * R, :] = pick((gae + tok_recv[c, 1]) * valid_out[c])
        adv_ref[c * R:(c + 1) * R, :] = pick((gae - mean) * valid_out[c] * scale)

    for o in range(owners):
        @pl.when(base + o != s)
        def _():
            part_copy(o).wait_send()

    @pl.when(rw_at != s)
    def _():
        rw_copy().wait_send()

    for entry in infos:
        info_copy(*entry).wait_send()

    @pl.when(is_owner)
    def _():
        for h in range(per):
            for c in range(nb):
                @pl.when((mine * per + h != s) | (b != c))
                def _():
                    tok_copy(h, c).wait_send()
        if everyone <= 32:
            for k in range(1, everyone):
                sum_copy(k).wait_send()
        else:
            def finish(k, carry):
                sum_copy(k).wait_send()
                return carry
            lax.fori_loop(1, everyone, finish, 0)


def per_device(hidden, gain, weight, rewards, mask, lengths, horizon):
    n = lax.axis_size("seq")
    nb = lax.axis_size("batch")
    owners = n // 2 if n % 4 == 0 else n
    R, T, depth = hidden.shape
    block = rewards.shape[1]
    per = n // owners
    G = T // owners // LANES
    gb = block // LANES
    rows = G * R
    everyone = n * nb
    dma = pltpu.SemaphoreType.DMA
    out = jax.ShapeDtypeStruct((R * nb, block // nb), F32)
    return pl.pallas_call(
        functools.partial(kernel, n, nb, owners),
        out_shape=(out, out),
        in_specs=[pl.BlockSpec(memory_space=pl.ANY)] * 7,
        out_specs=(pl.BlockSpec(memory_space=pltpu.VMEM),) * 2,
        scratch_shapes=[
            pltpu.VMEM((R, T, depth), jnp.bfloat16),
            pltpu.VMEM((depth,), F32),
            pltpu.VMEM((depth,), F32),
            pltpu.VMEM((R, block), F32),
            pltpu.VMEM((R, block), jnp.int32),
            pltpu.SMEM((R,), jnp.int32),
            pltpu.SMEM((R,), F32),
            pltpu.VMEM((owners, 2, rows, LANES), F32),
            pltpu.VMEM((n, 2, rows, LANES), F32),
            pltpu.VMEM((gb * R, LANES), F32),
            pltpu.VMEM((per, gb * R, LANES), F32),
            pltpu.VMEM((R, LANES), jnp.int32),
            pltpu.VMEM((nb, R, LANES), jnp.int32),
            pltpu.VMEM((R, LANES), F32),
            pltpu.VMEM((nb, R, LANES), F32),
            pltpu.VMEM((R, LANES), F32),
            pltpu.VMEM((owners, nb, R, LANES), F32),
            pltpu.VMEM((G, 2, R, LANES), F32),
            pltpu.VMEM((nb, 2, R, LANES), F32),
            dma((owners,)), dma((6,)),
            dma((owners,)), dma((n,)),
            dma(()), dma((per,)),
            dma((2, nb)), dma((2, nb)),
            dma((everyone,)), dma((owners, nb)),
            dma((per, nb)), dma((nb,)),
        ],
        compiler_params=pltpu.CompilerParams(collective_id=0, has_side_effects=True),
    )(hidden, gain, weight, rewards, mask, lengths, horizon)


def solution(mesh):
    return jax.shard_map(
        per_device,
        mesh=mesh,
        in_specs=(
            P("batch", None, "seq"),
            P("seq"),
            P("seq"),
            P("batch", "seq"),
            P("batch", "seq"),
            P("batch"),
            P("batch"),
        ),
        out_specs=(P(None, ("seq", "batch")), P(None, ("seq", "batch"))),
        check_vma=False,
    )
```

```python
import functools

import jax
import jax.numpy as jnp
from jax import lax
from jax.experimental import pallas as pl
from jax.experimental.pallas import tpu as pltpu
from jax.sharding import PartitionSpec as P

EPS = 1e-05
LANES = 128
F32 = jnp.float32


def kernel(n, nb, owners, hidden, gain, weight, rewards, mask, lengths, horizon,
           out_ref,
           hv, gain_v, weight_v, rew_v, mask_v, len_s, hor_s,
           part, rbuf, rw_send, rw_recv, len_send, len_recv, hor_send, hor_recv,
           sum_send, sum_recv, tok_send, tok_recv,
           chunk_sem, small_sem, part_ss, part_rs, rw_ss, rw_rs, info_ss, info_rs,
           sum_ss, sum_rs, tok_ss, tok_rs):
    R, T, depth = hidden.shape
    block = rewards.shape[1]
    width = block // nb
    per = n // owners
    base = (n - owners) // 2
    L = T // owners
    G = L // LANES
    gb = block // LANES
    rows = G * R
    total = depth * n
    everyone = n * nb
    s = lax.axis_index("seq")
    b = lax.axis_index("batch")
    is_owner = (s >= base) & (s < base + owners)
    mine = s - base
    out_o = s // per
    rw_at = base + out_o
    half = s % per

    def chunk_copy(o):
        span = pl.ds(o * L, L)
        return pltpu.make_async_copy(hidden.at[:, span, :], hv.at[:, span, :], chunk_sem.at[o])

    smalls = [
        pltpu.make_async_copy(src, dst, small_sem.at[i])
        for i, (src, dst) in enumerate(
            ((gain, gain_v), (weight, weight_v), (rewards, rew_v), (mask, mask_v),
             (lengths, len_s), (horizon, hor_s)))
    ]
    for copy in smalls:
        copy.start()
    near_high = s * (owners // 2) // n
    near_low = s % 2

    def turn(k):
        back = owners - 1 - k
        if owners % 2:
            return (s + back) % owners
        return (near_high + back // 2) % (owners // 2) * 2 + (near_low + back) % 2

    for k in range(owners):
        chunk_copy(turn(k)).start()
    barrier = pltpu.get_barrier_semaphore()
    for k in range(1, n):
        peer = (s + k) % n

        @pl.when(is_owner | ((peer >= base) & (peer < base + owners)))
        def _():
            pl.semaphore_signal(barrier, inc=1, device_id={"seq": peer},
                                device_id_type=pl.DeviceIdType.MESH)
    for k in range(1, nb):
        pl.semaphore_signal(barrier, inc=1, device_id={"batch": (b + k) % nb},
                            device_id_type=pl.DeviceIdType.MESH)
    for copy in smalls:
        copy.wait()

    head = (gain_v[...] * weight_v[...]).reshape(1, depth)
    high = head.astype(jnp.bfloat16).astype(F32)
    middle = (head - high).astype(jnp.bfloat16).astype(F32)
    low = head - high - middle
    wrow = lax.broadcasted_iota(jnp.int32, (16, depth), 0)
    pieces = jnp.where(wrow == 0, high, jnp.where(wrow == 1, middle, jnp.where(wrow == 2, low, 0.0)))
    pieces = pieces.astype(jnp.bfloat16)

    rw = rew_v[...] * mask_v[...].astype(F32)
    for g in range(gb):
        rw_send[g * R:(g + 1) * R, :] = rw[:, g * LANES:(g + 1) * LANES]
    for r in range(R):
        len_send[r:r + 1, :] = jnp.full((1, LANES), len_s[r], jnp.int32)
        hor_send[r:r + 1, :] = jnp.full((1, LANES), hor_s[r], F32)

    diagonal = (lax.broadcasted_iota(jnp.int32, (LANES, LANES), 0)
                == lax.broadcasted_iota(jnp.int32, (LANES, LANES), 1))

    infos = []
    for k in range(1, nb):
        for i, (src, dst) in enumerate(((len_send, len_recv), (hor_send, hor_recv))):
            infos.append((k, i, src, dst))

    def info_copy(k, i, src, dst):
        return pltpu.make_async_remote_copy(
            src, dst.at[b], info_ss.at[i, k], info_rs.at[i, b],
            device_id={"batch": (b + k) % nb}, device_id_type=pl.DeviceIdType.MESH)

    def info_arrived(k, i, src, dst):
        at = (b + k) % nb
        return pltpu.make_async_remote_copy(
            src, dst.at[at], info_ss.at[i, k], info_rs.at[i, at],
            device_id={"batch": at}, device_id_type=pl.DeviceIdType.MESH)

    def part_copy(o):
        return pltpu.make_async_remote_copy(
            part.at[o], rbuf.at[s], part_ss.at[o], part_rs.at[s],
            device_id={"seq": base + o}, device_id_type=pl.DeviceIdType.MESH)

    def rw_copy():
        return pltpu.make_async_remote_copy(
            rw_send, rw_recv.at[half], rw_ss, rw_rs.at[half],
            device_id={"seq": rw_at}, device_id_type=pl.DeviceIdType.MESH)

    def send_part(o):
        @pl.when(base + o != s)
        def _():
            part_copy(o).start()

    meet = min(1, owners - 1)

    def compute(k, carry):
        o = turn(k)
        chunk_copy(o).wait()
        for g in range(G):
            for r in range(R):
                at = pl.ds(pl.multiple_of(o * L + g * LANES, LANES), LANES)
                h = hv[r, at, :]
                both = lax.dot_general(jnp.concatenate([h, pieces], 0), h,
                                       (((1,), (1,)), ((), ())), preferred_element_type=F32)
                row = g * R + r
                part[o, 0, row:row + 1, :] = jnp.sum(both[LANES:LANES + 8], 0, keepdims=True)
                part[o, 1, row:row + 1, :] = jnp.sum(
                    jnp.where(diagonal, both[:LANES], 0.0), 0, keepdims=True)

        @pl.when(k == meet)
        def _():
            met = jnp.where(is_owner, n - 1, owners) + nb - 1
            pl.semaphore_wait(barrier, met)
            for before in range(meet):
                send_part(turn(before))

            @pl.when(rw_at != s)
            def _():
                rw_copy().start()

            for entry in infos:
                info_copy(*entry).start()

        @pl.when(k >= meet)
        def _():
            send_part(o)
        return carry

    lax.fori_loop(0, owners, compute, 0)

    @pl.when(rw_at == s)
    def _():
        rw_recv[half] = rw_send[...]

    len_recv[b] = len_send[...]
    hor_recv[b] = hor_send[...]

    def sum_copy(k):
        to = (s * nb + b + k) % everyone
        return pltpu.make_async_remote_copy(
            sum_send, sum_recv.at[mine, b], sum_ss.at[k], sum_rs.at[mine, b],
            device_id={"seq": to // nb, "batch": to % nb}, device_id_type=pl.DeviceIdType.MESH)

    def tok_copy(h, c):
        g = h * gb + (c * width) // LANES
        return pltpu.make_async_remote_copy(
            tok_send.at[g], tok_recv.at[b], tok_ss.at[h, c], tok_rs.at[b],
            device_id={"seq": mine * per + h, "batch": c}, device_id_type=pl.DeviceIdType.MESH)

    @pl.when(is_owner)
    def _():
        row = lax.broadcasted_iota(jnp.int32, (rows, LANES), 0)
        lane = lax.broadcasted_iota(jnp.int32, (rows, LANES), 1)
        group = row // R
        which = row % R
        length = jnp.full((rows, LANES), len_s[0], jnp.int32)
        reach = jnp.full((rows, LANES), hor_s[0], F32)
        for r in range(1, R):
            length = jnp.where(which == r, len_s[r], length)
            reach = jnp.where(which == r, hor_s[r], reach)
        rate = -1.0 / reach
        local = group * LANES + lane
        token = mine * L + local
        valid = (token < length).astype(F32)
        next_valid = (token + 1 < length).astype(F32)
        steps = [1 << i for i in range(LANES.bit_length() - 1)]
        lane_decay = [jnp.where(lane < LANES - k, jnp.exp(rate * k), 0.0) for k in steps]
        hops = [1 << i for i in range(max(G - 1, 0).bit_length())]
        row_decay = [jnp.where(group + k < G, jnp.exp(rate * (k * LANES)), 0.0) for k in hops]
        into = jnp.where(group < G - 1, jnp.exp(rate * (LANES - lane).astype(F32)), 0.0)
        power = jnp.exp(rate * (L - 1 - local).astype(F32))
        decay = jnp.exp(rate)
        power_sum = jnp.sum(power, 1, keepdims=True)
        power_squares = jnp.sum(power * power, 1, keepdims=True)

        for h in range(per):
            @pl.when(mine * per + h != s)
            def _():
                pltpu.make_async_remote_copy(
                    rw_send, rw_recv.at[h], rw_ss, rw_rs.at[h],
                    device_id={"seq": s}, device_id_type=pl.DeviceIdType.MESH).wait_recv()
        gains = jnp.concatenate([rw_recv[h] for h in range(per)], 0)

        rbuf[s] = part[mine]
        for k in range(1, n):
            at = (s + k) % n
            pltpu.make_async_remote_copy(
                part.at[0], rbuf.at[at], part_ss.at[0], part_rs.at[at],
                device_id={"seq": at}, device_id_type=pl.DeviceIdType.MESH).wait_recv()
        projected = rbuf[0, 0]
        squares = rbuf[0, 1]
        for k in range(1, n):
            projected = projected + rbuf[k, 0]
            squares = squares + rbuf[k, 1]
        values = projected * lax.rsqrt(squares / total + EPS)
        ahead = pltpu.roll(values, LANES - 1, 1)
        if G > 1:
            after = jnp.where(group < G - 1, pltpu.roll(ahead, rows - R, 0), 0.0)
        else:
            after = jnp.zeros_like(ahead)
        next_values = jnp.where(lane == LANES - 1, after, ahead)
        gae = (gains + next_valid * next_values - values) * valid
        for k, factor in zip(steps, lane_decay):
            gae = gae + factor * pltpu.roll(gae, LANES - k, 1)
        if G > 1:
            start = jnp.broadcast_to(gae[:, 0:1], (rows, LANES))
            for k, factor in zip(hops, row_decay):
                start = start + factor * pltpu.roll(start, rows - k * R, 0)
            gae = gae + into * pltpu.roll(start, rows - R, 0)
        for g in range(G):
            tok_send[g, 0] = gae[g * R:(g + 1) * R]
            tok_send[g, 1] = values[g * R:(g + 1) * R]
        for h in range(per):
            for c in range(nb):
                self_copy = (mine * per + h == s) & (b == c)

                @pl.when(jnp.logical_not(self_copy))
                def _():
                    tok_copy(h, c).start()

                @pl.when(self_copy)
                def _():
                    tok_recv[b] = tok_send[h * gb + (c * width) // LANES]
        sums = jnp.where(lane == 1, jnp.sum(gae, 1, keepdims=True), 0.0)
        sums = jnp.where(lane == 2, 2.0 * jnp.sum(gae * power, 1, keepdims=True), sums)
        sums = jnp.where(lane == 3, jnp.sum(gae * gae, 1, keepdims=True), sums)
        sums = jnp.where(lane == 4, power_sum, sums)
        sums = jnp.where(lane == 5, power_squares, sums)
        sums = jnp.where((lane == 0) & (group == 0), values + decay * gae, sums)
        summary = sums[0:R]
        for g in range(1, G):
            summary = summary + sums[g * R:(g + 1) * R]
        sum_send[...] = summary
        sum_recv[mine, b] = summary
        if everyone <= 32:
            for k in range(1, everyone):
                sum_copy(k).start()
        else:
            def start(k, carry):
                sum_copy(k).start()
                return carry
            lax.fori_loop(1, everyone, start, 0)

    for entry in infos:
        info_arrived(*entry).wait_recv()
    lane = lax.broadcasted_iota(jnp.int32, (R, LANES), 1)
    group_out = half * gb + (b * width) // LANES
    local = group_out * LANES + lane
    token = out_o * L + local
    count = jnp.zeros((R, LANES), F32)
    jump, power_out, valid_out, lens = [], [], [], []
    for c in range(nb):
        length = len_recv[c]
        rate = -1.0 / hor_recv[c]
        count = count + jnp.minimum(length, T).astype(F32)
        jump.append(jnp.exp(rate * float(L)))
        power_out.append(jnp.exp(rate * (L - 1 - local).astype(F32)))
        valid_out.append((token < length).astype(F32))
        lens.append(length)
    count = jnp.sum(count, 0, keepdims=True)

    for o in range(owners):
        for c in range(nb):
            @pl.when((base + o != s) | (b != c))
            def _():
                pltpu.make_async_remote_copy(
                    sum_send, sum_recv.at[o, c], sum_ss.at[0], sum_rs.at[o, c],
                    device_id={"seq": base + o, "batch": c},
                    device_id_type=pl.DeviceIdType.MESH).wait_recv()

    acc = jnp.zeros((R, LANES), F32)
    entering = []
    for c in range(nb):
        u = jnp.zeros((R, LANES), F32)
        chosen = jnp.zeros((R, LANES), F32)
        for o in reversed(range(owners)):
            message = sum_recv[o, c]
            factor = jnp.where((lane == 1) | (lane == 3), 1.0,
                               jnp.where((lane == 2) | (lane == 4), u,
                                         jnp.where(lane == 5, u * u, 0.0)))
            acc = acc + message * factor
            chosen = jnp.where(out_o == o, u, chosen)
            if o:
                first_value = jnp.broadcast_to(message[:, 0:1], (R, LANES))
                u = jnp.where(o * L < lens[c], first_value + jump[c] * u, 0.0)
        entering.append(chosen)
    acc = jnp.sum(acc, 0, keepdims=True)
    lane1 = lax.broadcasted_iota(jnp.int32, (1, LANES), 1)
    first = jnp.sum(jnp.where((lane1 == 1) | (lane1 == 4), acc, 0.0), 1, keepdims=True)
    second = jnp.sum(jnp.where((lane1 == 2) | (lane1 == 3) | (lane1 == 5), acc, 0.0), 1, keepdims=True)
    mean = first / count
    var = jnp.maximum(second / count - mean * mean, 1.0)
    scale = lax.rsqrt(var)

    for c in range(nb):
        @pl.when((rw_at != s) | (b != c))
        def _():
            pltpu.make_async_remote_copy(
                tok_send.at[0], tok_recv.at[c], tok_ss.at[0, 0], tok_rs.at[c],
                device_id={"seq": rw_at, "batch": c},
                device_id_type=pl.DeviceIdType.MESH).wait_recv()
    spots = LANES // width
    spot = b % spots

    def pick(x):
        result = x[:, 0:width]
        for j in range(1, spots):
            result = jnp.where(spot == j, x[:, j * width:(j + 1) * width], result)
        return result

    for c in range(nb):
        gae = tok_recv[c, 0] + power_out[c] * entering[c]
        out_ref[(nb + c) * R:(nb + c + 1) * R, :] = pick((gae + tok_recv[c, 1]) * valid_out[c])
        out_ref[c * R:(c + 1) * R, :] = pick((gae - mean) * valid_out[c] * scale)

    for o in range(owners):
        @pl.when(base + o != s)
        def _():
            part_copy(o).wait_send()

    @pl.when(rw_at != s)
    def _():
        rw_copy().wait_send()

    for entry in infos:
        info_copy(*entry).wait_send()

    @pl.when(is_owner)
    def _():
        for h in range(per):
            for c in range(nb):
                @pl.when((mine * per + h != s) | (b != c))
                def _():
                    tok_copy(h, c).wait_send()
        if everyone <= 32:
            for k in range(1, everyone):
                sum_copy(k).wait_send()
        else:
            def finish(k, carry):
                sum_copy(k).wait_send()
                return carry
            lax.fori_loop(1, everyone, finish, 0)


def per_device(hidden, gain, weight, rewards, mask, lengths, horizon):
    n = lax.axis_size("seq")
    nb = lax.axis_size("batch")
    owners = n // 2 if n % 4 == 0 else n
    R, T, depth = hidden.shape
    block = rewards.shape[1]
    per = n // owners
    G = T // owners // LANES
    gb = block // LANES
    rows = G * R
    everyone = n * nb
    dma = pltpu.SemaphoreType.DMA
    both = pl.pallas_call(
        functools.partial(kernel, n, nb, owners),
        out_shape=pltpu.VMEM((2 * R * nb, block // nb), F32),
        in_specs=[pl.BlockSpec(memory_space=pl.ANY)] * 7,
        out_specs=pl.BlockSpec(memory_space=pltpu.VMEM),
        scratch_shapes=[
            pltpu.VMEM((R, T, depth), jnp.bfloat16),
            pltpu.VMEM((depth,), F32),
            pltpu.VMEM((depth,), F32),
            pltpu.VMEM((R, block), F32),
            pltpu.VMEM((R, block), jnp.int32),
            pltpu.SMEM((R,), jnp.int32),
            pltpu.SMEM((R,), F32),
            pltpu.VMEM((owners, 2, rows, LANES), F32),
            pltpu.VMEM((n, 2, rows, LANES), F32),
            pltpu.VMEM((gb * R, LANES), F32),
            pltpu.VMEM((per, gb * R, LANES), F32),
            pltpu.VMEM((R, LANES), jnp.int32),
            pltpu.VMEM((nb, R, LANES), jnp.int32),
            pltpu.VMEM((R, LANES), F32),
            pltpu.VMEM((nb, R, LANES), F32),
            pltpu.VMEM((R, LANES), F32),
            pltpu.VMEM((owners, nb, R, LANES), F32),
            pltpu.VMEM((G, 2, R, LANES), F32),
            pltpu.VMEM((nb, 2, R, LANES), F32),
            dma((owners,)), dma((6,)),
            dma((owners,)), dma((n,)),
            dma(()), dma((per,)),
            dma((2, nb)), dma((2, nb)),
            dma((everyone,)), dma((owners, nb)),
            dma((per, nb)), dma((nb,)),
        ],
        compiler_params=pltpu.CompilerParams(collective_id=0, has_side_effects=True),
    )(hidden, gain, weight, rewards, mask, lengths, horizon)
    return both[:R * nb], both[R * nb:]


def solution(mesh):
    return jax.shard_map(
        per_device,
        mesh=mesh,
        in_specs=(
            P("batch", None, "seq"),
            P("seq"),
            P("seq"),
            P("batch", "seq"),
            P("batch", "seq"),
            P("batch"),
            P("batch"),
        ),
        out_specs=(P(None, ("seq", "batch")), P(None, ("seq", "batch"))),
        check_vma=False,
    )
```

```python
import functools

import jax
import jax.numpy as jnp
from jax import lax
from jax.experimental import pallas as pl
from jax.experimental.pallas import tpu as pltpu
from jax.sharding import PartitionSpec as P

EPS = 1e-05
LANES = 128
F32 = jnp.float32


def kernel(n, nb, owners, hidden, gain, weight, rewards, mask, lengths, horizon,
           out_ref,
           hv, gain_v, weight_v, rew_v, mask_v, len_s, hor_s,
           part, rbuf, rw_send, rw_recv, len_send, len_recv, hor_send, hor_recv,
           sum_send, sum_recv, tok_send, tok_recv,
           chunk_sem, small_sem, part_ss, part_rs, rw_ss, rw_rs, info_ss, info_rs,
           sum_ss, sum_rs, tok_ss, tok_rs):
    R, T, depth = hidden.shape
    block = rewards.shape[1]
    width = block // nb
    per = n // owners
    base = (n - owners) // 2
    L = T // owners
    G = L // LANES
    gb = block // LANES
    rows = G * R
    total = depth * n
    s = lax.axis_index("seq")
    b = lax.axis_index("batch")
    is_owner = (s >= base) & (s < base + owners)
    mine = s - base
    out_o = s // per
    rw_at = base + out_o
    half = s % per

    def chunk_copy(o, r):
        span = pl.ds(o * L, L)
        return pltpu.make_async_copy(hidden.at[r, span, :], hv.at[r, span, :], chunk_sem.at[o, r])

    smalls = [
        pltpu.make_async_copy(src, dst, small_sem.at[i])
        for i, (src, dst) in enumerate(
            ((gain, gain_v), (weight, weight_v), (rewards, rew_v), (mask, mask_v),
             (lengths, len_s), (horizon, hor_s)))
    ]
    for copy in smalls:
        copy.start()
    near_high = s * (owners // 2) // n
    near_low = s % 2

    def turn(k):
        back = owners - 1 - k
        if owners % 2:
            return (s + back) % owners
        return (near_high + back // 2) % (owners // 2) * 2 + (near_low + back) % 2

    for k in range(owners):
        for r in range(R):
            chunk_copy(turn(k), r).start()
    barrier = pltpu.get_barrier_semaphore()
    for k in range(1, n):
        peer = (s + k) % n

        @pl.when(is_owner | ((peer >= base) & (peer < base + owners)))
        def _():
            pl.semaphore_signal(barrier, inc=1, device_id={"seq": peer},
                                device_id_type=pl.DeviceIdType.MESH)
    for k in range(1, nb):
        pl.semaphore_signal(barrier, inc=1, device_id={"batch": lax.rem(b + k, nb)},
                            device_id_type=pl.DeviceIdType.MESH)
    for copy in smalls:
        copy.wait()

    head = (gain_v[...] * weight_v[...]).reshape(1, depth)
    high = head.astype(jnp.bfloat16).astype(F32)
    middle = (head - high).astype(jnp.bfloat16).astype(F32)
    low = head - high - middle
    wrow = lax.broadcasted_iota(jnp.int32, (16, depth), 0)
    pieces = jnp.where(wrow == 0, high, jnp.where(wrow == 1, middle, jnp.where(wrow == 2, low, 0.0)))
    pieces = pieces.astype(jnp.bfloat16)

    rw = rew_v[...] * mask_v[...].astype(F32)
    for g in range(gb):
        rw_send[g * R:(g + 1) * R, :] = rw[:, g * LANES:(g + 1) * LANES]
    for r in range(R):
        len_send[r:r + 1, :] = jnp.full((1, LANES), len_s[r], jnp.int32)
        hor_send[r:r + 1, :] = jnp.full((1, LANES), hor_s[r], F32)

    infos = []
    for k in range(1, nb):
        for i, (src, dst) in enumerate(((len_send, len_recv), (hor_send, hor_recv))):
            infos.append((k, i, src, dst))

    def info_copy(k, i, src, dst):
        return pltpu.make_async_remote_copy(
            src, dst.at[b], info_ss.at[i, k], info_rs.at[i, b],
            device_id={"batch": lax.rem(b + k, nb)}, device_id_type=pl.DeviceIdType.MESH)

    def info_arrived(k, i, src, dst):
        at = lax.rem(b + k, nb)
        return pltpu.make_async_remote_copy(
            src, dst.at[at], info_ss.at[i, k], info_rs.at[i, at],
            device_id={"batch": at}, device_id_type=pl.DeviceIdType.MESH)

    def part_copy(o):
        return pltpu.make_async_remote_copy(
            part.at[o], rbuf.at[s], part_ss.at[o], part_rs.at[s],
            device_id={"seq": base + o}, device_id_type=pl.DeviceIdType.MESH)

    def rw_copy():
        return pltpu.make_async_remote_copy(
            rw_send, rw_recv.at[half], rw_ss, rw_rs.at[half],
            device_id={"seq": rw_at}, device_id_type=pl.DeviceIdType.MESH)

    def send_part(o):
        @pl.when(base + o != s)
        def _():
            part_copy(o).start()

    meet = min(1, owners - 1)

    def compute(k, carry):
        o = turn(k)
        for r in range(R):
            chunk_copy(o, r).wait()
            for g in range(G):
                at = pl.ds(pl.multiple_of(o * L + g * LANES, LANES), LANES)
                h = hv[r, at, :]
                sums = lax.dot_general(pieces, h, (((1,), (1,)), ((), ())),
                                       preferred_element_type=F32)
                squares = jnp.zeros((LANES, LANES), F32)
                for j in range(depth // LANES):
                    wide = h[:, j * LANES:(j + 1) * LANES].astype(F32)
                    squares = squares + wide * wide
                row = g * R + r
                part[o, 0, row:row + 1, :] = jnp.sum(sums[0:8], 0, keepdims=True)
                part[o, 1, row:row + 1, :] = jnp.sum(squares.T, 0, keepdims=True)

        @pl.when(k == meet)
        def _():
            met = jnp.where(is_owner, n - 1, owners) + nb - 1
            pl.semaphore_wait(barrier, met)
            for before in range(meet):
                send_part(turn(before))

            @pl.when(rw_at != s)
            def _():
                rw_copy().start()

            for entry in infos:
                info_copy(*entry).start()

        @pl.when(k >= meet)
        def _():
            send_part(o)
        return carry

    lax.fori_loop(0, owners, compute, 0)

    @pl.when(rw_at == s)
    def _():
        rw_recv[half] = rw_send[...]

    len_recv[b] = len_send[...]
    hor_recv[b] = hor_send[...]

    def sum_copy(i, j):
        return pltpu.make_async_remote_copy(
            sum_send, sum_recv.at[mine, b], sum_ss.at[i, j], sum_rs.at[mine, b],
            device_id={"seq": i, "batch": j}, device_id_type=pl.DeviceIdType.MESH)

    def each_sum(act):
        def one(i):
            for j in range(nb):
                if isinstance(i, int) and not base <= i < base + owners:
                    act(sum_copy(i, j))
                else:
                    @pl.when((i != s) | (j != b))
                    def _():
                        act(sum_copy(i, j))

        if n * nb <= 32:
            for i in range(n):
                one(i)
        else:
            def body(i, carry):
                one(i)
                return carry
            lax.fori_loop(0, n, body, 0)

    def tok_copy(h, j):
        c = lax.rem(b + j, nb)
        g = h * gb + (c * width) // LANES
        return pltpu.make_async_remote_copy(
            tok_send.at[g], tok_recv.at[b], tok_ss.at[h, j], tok_rs.at[b],
            device_id={"seq": mine * per + h, "batch": c}, device_id_type=pl.DeviceIdType.MESH)

    def tok_local(h):
        g = h * gb + (b * width) // LANES
        return pltpu.make_async_copy(tok_send.at[g], tok_recv.at[b], tok_rs.at[b])

    @pl.when(is_owner)
    def _():
        row = lax.broadcasted_iota(jnp.int32, (rows, LANES), 0)
        lane = lax.broadcasted_iota(jnp.int32, (rows, LANES), 1)
        group = row // R
        which = row % R
        length = jnp.full((rows, LANES), len_s[0], jnp.int32)
        reach = jnp.full((rows, LANES), hor_s[0], F32)
        for r in range(1, R):
            length = jnp.where(which == r, len_s[r], length)
            reach = jnp.where(which == r, hor_s[r], reach)
        rate = -1.0 / reach
        local = group * LANES + lane
        token = mine * L + local
        valid = (token < length).astype(F32)
        next_valid = (token + 1 < length).astype(F32)
        levels = [[j * k for j in range(1, min(8, LANES // k))] for k in (1, 8, 64)]
        lane_decay = [[jnp.where(lane < LANES - k, jnp.exp(rate * k), 0.0) for k in level]
                      for level in levels]
        hops = [1 << i for i in range(max(G - 1, 0).bit_length())]
        row_decay = [jnp.where(group + k < G, jnp.exp(rate * (k * LANES)), 0.0) for k in hops]
        into = jnp.where(group < G - 1, jnp.exp(rate * (LANES - lane).astype(F32)), 0.0)
        power = jnp.exp(rate * (L - 1 - local).astype(F32))
        decay = jnp.exp(rate)
        power_sum = jnp.sum(power, 1, keepdims=True)
        power_squares = jnp.sum(power * power, 1, keepdims=True)

        for h in range(per):
            @pl.when(mine * per + h != s)
            def _():
                pltpu.make_async_remote_copy(
                    rw_send, rw_recv.at[h], rw_ss, rw_rs.at[h],
                    device_id={"seq": s}, device_id_type=pl.DeviceIdType.MESH).wait_recv()
        gains = jnp.concatenate([rw_recv[h] for h in range(per)], 0)

        rbuf[s] = part[mine]
        for k in range(1, n):
            at = (s + k) % n
            pltpu.make_async_remote_copy(
                part.at[0], rbuf.at[at], part_ss.at[0], part_rs.at[at],
                device_id={"seq": at}, device_id_type=pl.DeviceIdType.MESH).wait_recv()
        projected = rbuf[0, 0]
        squares = rbuf[0, 1]
        for k in range(1, n):
            projected = projected + rbuf[k, 0]
            squares = squares + rbuf[k, 1]
        values = projected * lax.rsqrt(squares / total + EPS)
        ahead = pltpu.roll(values, LANES - 1, 1)
        if G > 1:
            after = jnp.where(group < G - 1, pltpu.roll(ahead, rows - R, 0), 0.0)
        else:
            after = jnp.zeros_like(ahead)
        next_values = jnp.where(lane == LANES - 1, after, ahead)
        gae = (gains + next_valid * next_values - values) * valid
        for level, factors in zip(levels, lane_decay):
            terms = [factor * pltpu.roll(gae, LANES - k, 1) for k, factor in zip(level, factors)]
            gae = gae + sum(terms[1:], terms[0])
        if G > 1:
            start = jnp.broadcast_to(gae[:, 0:1], (rows, LANES))
            for k, factor in zip(hops, row_decay):
                start = start + factor * pltpu.roll(start, rows - k * R, 0)
            gae = gae + into * pltpu.roll(start, rows - R, 0)
        for g in range(G):
            tok_send[g, 0] = gae[g * R:(g + 1) * R]
            tok_send[g, 1] = values[g * R:(g + 1) * R]
        sums = jnp.where(lane == 1, jnp.sum(gae, 1, keepdims=True), 0.0)
        sums = jnp.where(lane == 2, 2.0 * jnp.sum(gae * power, 1, keepdims=True), sums)
        sums = jnp.where(lane == 3, jnp.sum(gae * gae, 1, keepdims=True), sums)
        sums = jnp.where(lane == 4, power_sum, sums)
        sums = jnp.where(lane == 5, power_squares, sums)
        sums = jnp.where((lane == 0) & (group == 0), values + decay * gae, sums)
        summary = sums[0:R]
        for g in range(1, G):
            summary = summary + sums[g * R:(g + 1) * R]
        sum_send[...] = summary
        pltpu.make_async_copy(sum_send, sum_recv.at[mine, b], sum_rs.at[mine, b]).start()
        each_sum(lambda copy: copy.start())
        for h in range(per):
            for j in range(1, nb):
                tok_copy(h, j).start()

            @pl.when(mine * per + h == s)
            def _():
                tok_local(h).start()

            @pl.when(mine * per + h != s)
            def _():
                tok_copy(h, 0).start()

    for o in range(owners):
        @pl.when(base + o != s)
        def _():
            part_copy(o).wait_send()

    @pl.when(rw_at != s)
    def _():
        rw_copy().wait_send()

    for entry in infos:
        info_copy(*entry).wait_send()

    for entry in infos:
        info_arrived(*entry).wait_recv()
    lane = lax.broadcasted_iota(jnp.int32, (R, LANES), 1)
    group_out = half * gb + (b * width) // LANES
    local = group_out * LANES + lane
    token = out_o * L + local
    count = jnp.zeros((R, LANES), F32)
    jump, power_out, valid_out, lens = [], [], [], []
    for c in range(nb):
        length = len_recv[c]
        rate = -1.0 / hor_recv[c]
        count = count + jnp.minimum(length, T).astype(F32)
        jump.append(jnp.exp(rate * float(L)))
        power_out.append(jnp.exp(rate * (L - 1 - local).astype(F32)))
        valid_out.append((token < length).astype(F32))
        lens.append(length)
    count = jnp.sum(count, 0, keepdims=True)

    @pl.when(is_owner)
    def _():
        each_sum(lambda copy: copy.wait_send())
        for h in range(per):
            for j in range(1, nb):
                tok_copy(h, j).wait_send()

            @pl.when(mine * per + h != s)
            def _():
                tok_copy(h, 0).wait_send()

    for o in range(owners):
        for c in range(nb):
            pltpu.make_async_remote_copy(
                sum_send, sum_recv.at[o, c], sum_ss.at[0, 0], sum_rs.at[o, c],
                device_id={"seq": base + o, "batch": c},
                device_id_type=pl.DeviceIdType.MESH).wait_recv()

    acc = jnp.zeros((R, LANES), F32)
    entering = []
    for c in range(nb):
        u = jnp.zeros((R, LANES), F32)
        chosen = jnp.zeros((R, LANES), F32)
        for o in reversed(range(owners)):
            message = sum_recv[o, c]
            factor = jnp.where((lane == 1) | (lane == 3), 1.0,
                               jnp.where((lane == 2) | (lane == 4), u,
                                         jnp.where(lane == 5, u * u, 0.0)))
            acc = acc + message * factor
            chosen = jnp.where(out_o == o, u, chosen)
            if o:
                first_value = jnp.broadcast_to(message[:, 0:1], (R, LANES))
                u = jnp.where(o * L < lens[c], first_value + jump[c] * u, 0.0)
        entering.append(chosen)
    acc = jnp.sum(acc, 0, keepdims=True)
    lane1 = lax.broadcasted_iota(jnp.int32, (1, LANES), 1)
    first = jnp.sum(jnp.where((lane1 == 1) | (lane1 == 4), acc, 0.0), 1, keepdims=True)
    second = jnp.sum(jnp.where((lane1 == 2) | (lane1 == 3) | (lane1 == 5), acc, 0.0), 1, keepdims=True)
    mean = first / count
    var = jnp.maximum(second / count - mean * mean, 1.0)
    scale = lax.rsqrt(var)

    for c in range(nb):
        pltpu.make_async_remote_copy(
            tok_send.at[0], tok_recv.at[c], tok_ss.at[0, 0], tok_rs.at[c],
            device_id={"seq": rw_at, "batch": c},
            device_id_type=pl.DeviceIdType.MESH).wait_recv()
    spots = LANES // width
    spot = b % spots

    def pick(x):
        result = x[:, 0:width]
        for j in range(1, spots):
            result = jnp.where(spot == j, x[:, j * width:(j + 1) * width], result)
        return result

    for c in range(nb):
        gae = tok_recv[c, 0] + power_out[c] * entering[c]
        out_ref[(nb + c) * R:(nb + c + 1) * R, :] = pick((gae + tok_recv[c, 1]) * valid_out[c])
        out_ref[c * R:(c + 1) * R, :] = pick((gae - mean) * valid_out[c] * scale)


def per_device(hidden, gain, weight, rewards, mask, lengths, horizon):
    n = lax.axis_size("seq")
    nb = lax.axis_size("batch")
    owners = n // 2 if n % 4 == 0 else n
    R, T, depth = hidden.shape
    block = rewards.shape[1]
    per = n // owners
    G = T // owners // LANES
    gb = block // LANES
    rows = G * R
    dma = pltpu.SemaphoreType.DMA
    both = pl.pallas_call(
        functools.partial(kernel, n, nb, owners),
        out_shape=pltpu.VMEM((2 * R * nb, block // nb), F32),
        in_specs=[pl.BlockSpec(memory_space=pl.ANY)] * 7,
        out_specs=pl.BlockSpec(memory_space=pltpu.VMEM),
        scratch_shapes=[
            pltpu.VMEM((R, T, depth), jnp.bfloat16),
            pltpu.VMEM((depth,), F32),
            pltpu.VMEM((depth,), F32),
            pltpu.VMEM((R, block), F32),
            pltpu.VMEM((R, block), jnp.int32),
            pltpu.SMEM((R,), jnp.int32),
            pltpu.SMEM((R,), F32),
            pltpu.VMEM((owners, 2, rows, LANES), F32),
            pltpu.VMEM((n, 2, rows, LANES), F32),
            pltpu.VMEM((gb * R, LANES), F32),
            pltpu.VMEM((per, gb * R, LANES), F32),
            pltpu.VMEM((R, LANES), jnp.int32),
            pltpu.VMEM((nb, R, LANES), jnp.int32),
            pltpu.VMEM((R, LANES), F32),
            pltpu.VMEM((nb, R, LANES), F32),
            pltpu.VMEM((R, LANES), F32),
            pltpu.VMEM((owners, nb, R, LANES), F32),
            pltpu.VMEM((G, 2, R, LANES), F32),
            pltpu.VMEM((nb, 2, R, LANES), F32),
            dma((owners, R)), dma((6,)),
            dma((owners,)), dma((n,)),
            dma(()), dma((per,)),
            dma((2, nb)), dma((2, nb)),
            dma((n, nb)), dma((owners, nb)),
            dma((per, nb)), dma((nb,)),
        ],
        compiler_params=pltpu.CompilerParams(collective_id=0, has_side_effects=True),
    )(hidden, gain, weight, rewards, mask, lengths, horizon)
    return both[:R * nb], both[R * nb:]


def solution(mesh):
    return jax.shard_map(
        per_device,
        mesh=mesh,
        in_specs=(
            P("batch", None, "seq"),
            P("seq"),
            P("seq"),
            P("batch", "seq"),
            P("batch", "seq"),
            P("batch"),
            P("batch"),
        ),
        out_specs=(P(None, ("seq", "batch")), P(None, ("seq", "batch"))),
        check_vma=False,
    )
```
